32 devices in a mesh: row: 4 (over z), col: 8 (over y, x, core).
Axes of the slice: x: 2, y: 2, z: 4, core: 2. Of those that a mesh axis runs over, the one named last changes fastest.
Arguments:
- factor_wide: float32 [4, 4, 2, 8, 512, 512], P(None, 'row', None, 'col'), may hold values from -1 to 2, as said below
- factor_narrow: bfloat16 [4, 4, 2, 8, 512, 512], P(None, 'row', None, 'col'), may hold values from -1 to 2, as said below
- flags: int32 [4, 4, 2, 8], P(None, 'row', None, 'col'), may hold values from 0 to 1
- forward_solution: float32 [2, 8, 512, 128], P(None, 'col'), may hold values from -0.5 to 0.5
- solution_grad: float32 [2, 8, 512, 128], P(None, 'col'), may hold values from -1.8 to 1.8
Outputs:
- rhs_grad: float32 [4, 4, 512, 128], P(None, 'row')
- factor_grad: float32 [4, 4, 2, 8, 512, 512], P(None, 'row', None, 'col')
The draws below stay inside these ranges and needn't reach their ends.
Inputs may be any that keep to these rules, and one draw needn't show every extreme that they name: `factor_wide`: the diagonal entries of every diagonal tile lie between 1 and 2. `factor_narrow`: the diagonal entries of every diagonal tile lie between 1 and 2.
All inputs are finite; a program needn't handle non-finite values.
Results may differ from the reference program's by a relative error of at most 0.0003.
Values sent between devices are 32-bit elements; how exact they have to be, the bound alone decides.
A program may use at most 64 MiB of HBM per device.

```python
import math
import jax
import jax.numpy as jnp
from jax import lax

TB = 512
NT = 16
R = 128
N_ROW = 4
N_COL = 8


coupling = 3.0


def factor_law(key):
    shape = (NT // N_ROW, N_ROW, NT // N_COL, N_COL, TB, TB)
    spread = jax.random.normal(key, shape, jnp.float32)
    diagonal = jax.random.uniform(jax.random.fold_in(key, 5), shape, jnp.float32, 1.0, 2.0)
    scaled = spread * (coupling / math.sqrt(NT * TB))
    row_shape = (NT // N_ROW, N_ROW, 1, 1, 1, 1)
    col_shape = (1, 1, NT // N_COL, N_COL, 1, 1)
    inner_shape = (1, 1, 1, 1, TB, TB)
    tile_row = lax.broadcasted_iota(jnp.int32, row_shape, 0) * N_ROW + lax.broadcasted_iota(jnp.int32, row_shape, 1)
    tile_col = lax.broadcasted_iota(jnp.int32, col_shape, 2) * N_COL + lax.broadcasted_iota(jnp.int32, col_shape, 3)
    inner_row = lax.broadcasted_iota(jnp.int32, inner_shape, 4)
    inner_col = lax.broadcasted_iota(jnp.int32, inner_shape, 5)
    on_diagonal = (tile_row == tile_col) & (inner_row == inner_col)
    return jnp.where(on_diagonal, diagonal, scaled)


def draw_factor_wide(key, part):
    return factor_law(jax.random.fold_in(key, 11))


def draw_factor_narrow(key, part):
    return factor_law(jax.random.fold_in(key, 23)).astype(jnp.bfloat16)


def with_ends(entries, rng, smallest, high):
    longest = entries.shape.index(max(entries.shape))
    spots = []
    for shift in (0, 1):
        where = [jax.random.randint(jax.random.fold_in(rng, axis), (), 0, length) for axis, length in enumerate(entries.shape)]
        where[longest] = (where[longest] + shift) % entries.shape[longest]
        spots.append(tuple(where))
    return entries.at[spots[0]].set(smallest).at[spots[1]].set(high)


def block_scale(rng, shape, split, low, high):
    loudness = 1.0
    for position, shards_of in split:
        heights = jax.random.uniform(jax.random.fold_in(jax.random.fold_in(rng, 6), position), (shards_of,), jnp.float32, low / len(split), high / len(split))
        loudness = loudness * jnp.repeat(jnp.exp(heights), shape[position] // shards_of).reshape((-1,) + (1,) * (len(shape) - 1 - position))
    return loudness


def normal_values(stream_key, shape, width, most, cuts=(), held_as=jnp.bfloat16):
    drawn = jax.random.normal(stream_key, shape, jnp.float32) * width
    if len(cuts) > 0:
        drawn = block_scale(stream_key, shape, cuts, -0.22, 0.18) * drawn
    return jnp.clip(drawn, min=-most, max=most).astype(held_as)


def setup_inputs(seed: int = 0) -> dict:
    seeds = jax.random.split(jax.random.key(seed), 6)
    factor_wide = draw_factor_wide(jax.random.fold_in(seeds[5], 71), 0)
    factor_narrow = draw_factor_narrow(jax.random.fold_in(seeds[5], 71), 0)
    flags = with_ends(jax.random.randint(seeds[2], (NT // N_ROW, N_ROW, NT // N_COL, N_COL), 0, 2), jax.random.fold_in(seeds[2], 1), 0, 1).astype(jnp.int32)
    forward_solution = normal_values(seeds[3], (NT // N_COL, N_COL, TB, R), R ** -0.5, 0.5, ((1, 8),), jnp.float32)
    solution_grad = normal_values(seeds[4], (NT // N_COL, N_COL, TB, R), 0.3, 1.8, ((1, 8),), jnp.float32)
    return {"factor_wide": factor_wide, "factor_narrow": factor_narrow, "flags": flags, "forward_solution": forward_solution, "solution_grad": solution_grad}


HIGHEST_PRECISION = lax.Precision.HIGHEST

def lower_mask(row_index, col_index, tile_width):
    inner_mask = lax.broadcasted_iota(jnp.int32, (tile_width, tile_width), 0) >= lax.broadcasted_iota(jnp.int32, (tile_width, tile_width), 1)
    return (row_index > col_index) | (row_index == col_index) & inner_mask

def reference(factor_wide, factor_narrow, flags, forward_solution, solution_grad):
    chosen = jnp.where(flags[:, :, :, :, None, None] == 1, factor_narrow.astype(jnp.float32), factor_wide)
    factor_tiles = chosen.reshape(NT, NT, TB, TB)
    solution_tiles = forward_solution.reshape(NT, TB, R)
    target_tiles = solution_grad.reshape(NT, TB, R)
    solved_tiles = [None] * NT
    for target in range(NT - 1, -1, -1):
        right_side = target_tiles[target]
        for source in range(target + 1, NT):
            right_side = right_side - jnp.dot(factor_tiles[source, target].T.astype(jnp.float32), solved_tiles[source].astype(jnp.float32), precision=HIGHEST_PRECISION, preferred_element_type=jnp.float32)
        solved_tiles[target] = lax.linalg.triangular_solve(factor_tiles[target, target], right_side, left_side=True, lower=True, transpose_a=True)
    rhs_grad = jnp.stack(solved_tiles)
    products = -jnp.einsum('akr,blr->abkl', rhs_grad, solution_tiles, precision=HIGHEST_PRECISION)
    tile_index = jnp.arange(NT, dtype=jnp.int32)
    masks = lower_mask(tile_index[:, None, None, None], tile_index[None, :, None, None], TB)
    factor_grad = jnp.where(masks, products, jnp.zeros_like(products))
    return (rhs_grad.reshape(NT // N_ROW, N_ROW, TB, R), factor_grad.reshape(NT // N_ROW, N_ROW, NT // N_COL, N_COL, TB, TB))
```

```python
import functools

import jax
import jax.numpy as jnp
from jax import lax
from jax.experimental import pallas as pl
from jax.experimental.pallas import tpu as pltpu
from jax.sharding import PartitionSpec as P

HIGHEST_PRECISION = lax.Precision.HIGHEST
PRODUCT_PRECISION = lax.Precision.HIGH
BASE_BLOCK = 128
MESH = pl.DeviceIdType.MESH


def lower_mask(row_index, col_index, tile_width):
    inner_mask = lax.broadcasted_iota(
        jnp.int32, (tile_width, tile_width), 0
    ) >= lax.broadcasted_iota(jnp.int32, (tile_width, tile_width), 1)
    return (row_index > col_index) | (row_index == col_index) & inner_mask


def matmul(a, b):
    return jnp.dot(a, b, precision=HIGHEST_PRECISION, preferred_element_type=jnp.float32)


def invert_kernel(tile_ref, inverse_ref):
    width = tile_ref.shape[1]
    base = min(BASE_BLOCK, width)
    row = lax.broadcasted_iota(jnp.int32, (base, base), 0)
    col = lax.broadcasted_iota(jnp.int32, (base, base), 1)
    starts = range(0, width, base)
    blocks = [tile_ref[0, at:at + base, at:at + base] for at in starts]
    inverses = [jnp.where(row == col, 1.0 / jnp.where(row == col, b, 1.0), 0.0) for b in blocks]
    size = 1
    while size < base:
        corner = (row // (2 * size) == col // (2 * size)) & (row // size > col // size)
        halves = [matmul(x, jnp.where(corner, b, 0.0)) for x, b in zip(inverses, blocks)]
        inverses = [x - matmul(h, x) for x, h in zip(inverses, halves)]
        size *= 2
    inverse_ref[0] = jnp.zeros((width, width), jnp.float32)
    for at, x in zip(starts, inverses):
        inverse_ref[0, at:at + base, at:at + base] = x
    while size < width:
        for at in range(0, width, 2 * size):
            top, low = slice(at, at + size), slice(at + size, at + 2 * size)
            half = matmul(inverse_ref[0, low, low], tile_ref[0, low, top])
            inverse_ref[0, low, top] = -matmul(half, inverse_ref[0, top, top])
        size *= 2


def invert(tiles):
    block = pl.BlockSpec((1,) + tiles.shape[1:], lambda s: (s, 0, 0))
    return pl.pallas_call(
        invert_kernel,
        grid=(tiles.shape[0],),
        in_specs=[block],
        out_specs=block,
        out_shape=jax.ShapeDtypeStruct(tiles.shape, jnp.float32),
    )(tiles)


def sweep_kernel(
    rows, cols, tiles_ref, inverse_ref, below_ref, target_ref, solved_ref,
    chain, total, parts, chain_send, plane_send, part_send, chain_recv, plane_recv, part_recv,
):
    my_row, my_col = lax.axis_index("row"), lax.axis_index("col")
    local_rows, local_cols = tiles_ref.shape[0], tiles_ref.shape[1]
    count = local_rows * rows
    gaps = [d for d in range(2, rows + 2) if d != rows]

    def away(row_step, col_step):
        return (lax.rem(my_row + row_step + rows, rows), lax.rem(my_col + col_step + cols, cols))

    partners = [away(0, o) for o in range(1, cols)] + [away(o, 0) for o in range(1, rows)]
    partners += [away(1, 1), away(-1, -1)]
    barrier = pltpu.get_barrier_semaphore()
    for partner in partners:
        pl.semaphore_signal(barrier, inc=1, device_id=partner, device_id_type=MESH)
    pl.semaphore_wait(barrier, len(partners))

    total[...] = jnp.zeros_like(total)

    def chain_copy(slot, landing):
        return pltpu.make_async_remote_copy(
            src_ref=solved_ref.at[slot], dst_ref=chain.at[landing],
            send_sem=chain_send.at[slot], recv_sem=chain_recv.at[landing],
            device_id=away(-1, -1), device_id_type=MESH,
        )

    def plane_copy(slot, offset):
        return pltpu.make_async_remote_copy(
            src_ref=solved_ref.at[slot], dst_ref=solved_ref.at[slot],
            send_sem=plane_send.at[slot, offset], recv_sem=plane_recv.at[slot],
            device_id=away(0, -offset), device_id_type=MESH,
        )

    def part_copy(slot, where, gap):
        return pltpu.make_async_remote_copy(
            src_ref=total.at[slot], dst_ref=parts.at[slot, where],
            send_sem=part_send.at[slot], recv_sem=part_recv.at[slot, where],
            device_id=away((-gap) % rows, 0), device_id_type=MESH,
        )

    plane_order = list(range(2, cols)) + [1]

    def step(offset, carry):
        j = count - 1 - offset
        slot, col_slot = j // rows, j // cols
        on_plane = my_row == lax.rem(j, rows)
        owner = on_plane & (my_col == lax.rem(j, cols))

        @pl.when(owner)
        def _():
            total[col_slot] = target_ref[col_slot] - total[col_slot]
            for where, gap in enumerate(gaps):
                @pl.when(j + gap < count)
                def _():
                    part_copy(col_slot, where, gap).wait_recv()
                    total[col_slot] = total[col_slot] - parts[col_slot, where]
            solved_ref[slot] = matmul(total[col_slot], inverse_ref[col_slot])

            @pl.when(j + 1 < count)
            def _():
                chain_copy(slot, col_slot).wait_recv()
                solved_ref[slot] = solved_ref[slot] - matmul(chain[col_slot], below_ref[col_slot])

            @pl.when(j > 0)
            def _():
                chain_copy(slot, (j - 1) // cols).start()
            for o in plane_order:
                plane_copy(slot, o).start()

        @pl.when(on_plane & jnp.logical_not(owner))
        def _():
            plane_copy(slot, 1).wait_recv()

        @pl.when(on_plane)
        def _():
            for s in reversed(range(local_cols)):
                k = my_col + cols * s

                @pl.when(k < j - 1)
                def _():
                    total[s] = total[s] + matmul(solved_ref[slot], tiles_ref[slot, s])
                for where, gap in enumerate(gaps):
                    @pl.when(k == j - gap)
                    def _():
                        part_copy(s, where, gap).start()
        return carry

    lax.fori_loop(0, count, step, 0)

    def drain(offset, carry):
        j = count - 1 - offset
        slot = j // rows
        on_plane = my_row == lax.rem(j, rows)

        @pl.when(on_plane & (my_col == lax.rem(j, cols)))
        def _():
            @pl.when(j > 0)
            def _():
                chain_copy(slot, 0).wait_send()
            for o in plane_order:
                plane_copy(slot, o).wait_send()

        @pl.when(on_plane)
        def _():
            for s in range(local_cols):
                for where, gap in enumerate(gaps):
                    @pl.when(my_col + cols * s == j - gap)
                    def _():
                        part_copy(s, where, gap).wait_send()
        return carry

    lax.fori_loop(0, count, drain, 0)


def sweep(rows, cols, tiles, inverse, below, target):
    local_rows, local_cols, width = tiles.shape[0], tiles.shape[1], tiles.shape[2]
    rhs = target.shape[1]
    vmem = pl.BlockSpec(memory_space=pltpu.VMEM)
    dma = pltpu.SemaphoreType.DMA
    return pl.pallas_call(
        functools.partial(sweep_kernel, rows, cols),
        out_shape=jax.ShapeDtypeStruct((local_rows, rhs, width), jnp.float32),
        in_specs=[vmem] * 4,
        out_specs=vmem,
        scratch_shapes=[
            pltpu.VMEM((local_cols, rhs, width), jnp.float32),
            pltpu.VMEM((local_cols, rhs, width), jnp.float32),
            pltpu.VMEM((local_cols, rows - 1, rhs, width), jnp.float32),
            dma((local_rows,)),
            dma((local_rows, cols)),
            dma((local_cols,)),
            dma((local_cols,)),
            dma((local_rows,)),
            dma((local_cols, rows - 1)),
        ],
        compiler_params=pltpu.CompilerParams(collective_id=0, has_side_effects=True),
    )(tiles, inverse, below, target)


def body(factor_wide, factor_narrow, flags, forward_solution, solution_grad):
    row_count = lax.axis_size("row")
    col_count = lax.axis_size("col")
    my_row = lax.axis_index("row")
    my_col = lax.axis_index("col")
    local_rows = factor_wide.shape[0]
    local_cols = factor_wide.shape[2]
    tile_width = factor_wide.shape[4]
    tile_count = local_rows * row_count

    def pick(row_slot, col_slot):
        def cut(pool):
            return lax.dynamic_index_in_dim(pool[:, 0, col_slot, 0], row_slot, 0, keepdims=False)
        narrow = cut(flags) == 1
        return jnp.where(narrow, cut(factor_narrow).astype(jnp.float32), cut(factor_wide))

    targets = [my_col + col_count * s for s in range(local_cols)]
    below = jnp.stack([
        pick(jnp.minimum(j + 1, tile_count - 1) // row_count, s) for s, j in enumerate(targets)
    ])
    below = lax.ppermute(below, "row", [(i, (i - 1) % row_count) for i in range(row_count)])
    factor_tiles = jnp.where(
        flags[:, 0, :, 0, None, None] == 1,
        factor_narrow[:, 0, :, 0].astype(jnp.float32),
        factor_wide[:, 0, :, 0],
    )
    diagonal = jnp.stack([pick(j // row_count, s) for s, j in enumerate(targets)])
    inverse = invert(diagonal)
    correction = jnp.einsum(
        "sab,sbc->sac", below, inverse, precision=HIGHEST_PRECISION,
        preferred_element_type=jnp.float32,
    )
    target = jnp.swapaxes(solution_grad[:, 0], 1, 2)
    solved = sweep(row_count, col_count, factor_tiles, inverse, correction, target)
    row_index = jnp.arange(local_rows, dtype=jnp.int32) * row_count + my_row
    col_index = jnp.arange(local_cols, dtype=jnp.int32) * col_count + my_col
    products = -jnp.einsum(
        "ark,blr->abkl", solved, forward_solution[:, 0], precision=PRODUCT_PRECISION
    )
    masks = lower_mask(row_index[:, None, None, None], col_index[None, :, None, None], tile_width)
    factor_grad = jnp.where(masks, products, jnp.zeros_like(products))
    return (jnp.swapaxes(solved, 1, 2)[:, None], factor_grad[:, None, :, None])


def solution(mesh):
    placed = (
        P(None, "row", None, "col", None, None),
        P(None, "row", None, "col", None, None),
        P(None, "row", None, "col"),
        P(None, "col", None, None),
        P(None, "col", None, None),
    )
    return jax.shard_map(
        body,
        mesh=mesh,
        in_specs=placed,
        out_specs=(P(None, "row", None, None), P(None, "row", None, "col", None, None)),
        check_vma=False,
    )
```

```python
import functools

import jax
import jax.numpy as jnp
from jax import lax
from jax.experimental import pallas as pl
from jax.experimental.pallas import tpu as pltpu
from jax.sharding import PartitionSpec as P

HIGHEST_PRECISION = lax.Precision.HIGHEST
PRODUCT_PRECISION = lax.Precision.HIGH
BASE_BLOCK = 128
MESH = pl.DeviceIdType.MESH


def lower_mask(row_index, col_index, tile_width):
    inner_mask = lax.broadcasted_iota(
        jnp.int32, (tile_width, tile_width), 0
    ) >= lax.broadcasted_iota(jnp.int32, (tile_width, tile_width), 1)
    return (row_index > col_index) | (row_index == col_index) & inner_mask


def matmul(a, b):
    return jnp.dot(a, b, precision=HIGHEST_PRECISION, preferred_element_type=jnp.float32)


def split(value):
    high = value.astype(jnp.bfloat16)
    return high, (value - high.astype(jnp.float32)).astype(jnp.bfloat16)


def split_product(value, high, low):
    count = value.shape[0]
    value_high, value_low = split(value)
    both = jnp.concatenate([value_high, value_low], axis=0)
    first = jnp.dot(both, high, preferred_element_type=jnp.float32)
    second = jnp.dot(value_high, low, preferred_element_type=jnp.float32)
    return first[:count] + (first[count:] + second)


def invert_kernel(tile_ref, inverse_ref):
    width = tile_ref.shape[0]
    base = min(BASE_BLOCK, width)
    row = lax.broadcasted_iota(jnp.int32, (base, base), 0)
    col = lax.broadcasted_iota(jnp.int32, (base, base), 1)
    starts = range(0, width, base)
    blocks = [tile_ref[at:at + base, at:at + base] for at in starts]
    inverses = [jnp.where(row == col, 1.0 / jnp.where(row == col, b, 1.0), 0.0) for b in blocks]
    size = 1
    while size < base:
        corner = (row // (2 * size) == col // (2 * size)) & (row // size > col // size)
        halves = [matmul(x, jnp.where(corner, b, 0.0)) for x, b in zip(inverses, blocks)]
        inverses = [x - matmul(h, x) for x, h in zip(inverses, halves)]
        size *= 2
    inverse_ref[...] = jnp.zeros((width, width), jnp.float32)
    for at, x in zip(starts, inverses):
        inverse_ref[at:at + base, at:at + base] = x
    while size < width:
        for at in range(0, width, 2 * size):
            top, low = slice(at, at + size), slice(at + size, at + 2 * size)
            half = matmul(inverse_ref[low, low], tile_ref[low, top])
            inverse_ref[low, top] = -matmul(half, inverse_ref[top, top])
        size *= 2


def invert(tile):
    return pl.pallas_call(
        invert_kernel, out_shape=jax.ShapeDtypeStruct(tile.shape, jnp.float32)
    )(tile)


def sweep_kernel(rows, cols, tiles_ref, target_ref, *refs):
    local_cols = tiles_ref.shape[1]
    inverse_refs, below_refs = refs[:local_cols], refs[local_cols:2 * local_cols]
    (
        solved_ref, chain, total, parts, weights, chain_send, plane_send, part_send,
        chain_recv, plane_recv, part_recv,
    ) = refs[2 * local_cols:]
    my_row, my_col = lax.axis_index("row"), lax.axis_index("col")
    local_rows = tiles_ref.shape[0]
    count = local_rows * rows
    gaps = [d for d in range(2, rows + 2) if d != rows]

    def away(row_step, col_step):
        return (lax.rem(my_row + row_step + rows, rows), lax.rem(my_col + col_step + cols, cols))

    partners = [away(0, o) for o in range(1, cols)] + [away(o, 0) for o in range(1, rows)]
    partners += [away(1, 1), away(-1, -1)]
    barrier = pltpu.get_barrier_semaphore()
    for partner in partners:
        pl.semaphore_signal(barrier, inc=1, device_id=partner, device_id_type=MESH)
    pl.semaphore_wait(barrier, len(partners))

    total[...] = jnp.zeros_like(total)
    for s in range(local_cols):
        weights[s, 0], weights[s, 1] = split(inverse_refs[s][...])
        weights[s, 2], weights[s, 3] = split(below_refs[s][...])

    def chain_copy(slot, landing):
        return pltpu.make_async_remote_copy(
            src_ref=solved_ref.at[slot], dst_ref=chain.at[landing],
            send_sem=chain_send.at[slot], recv_sem=chain_recv.at[landing],
            device_id=away(-1, -1), device_id_type=MESH,
        )

    def plane_copy(slot, offset):
        return pltpu.make_async_remote_copy(
            src_ref=solved_ref.at[slot], dst_ref=solved_ref.at[slot],
            send_sem=plane_send.at[slot, offset], recv_sem=plane_recv.at[slot],
            device_id=away(0, -offset), device_id_type=MESH,
        )

    def part_copy(slot, where, gap):
        return pltpu.make_async_remote_copy(
            src_ref=total.at[slot], dst_ref=parts.at[slot, where],
            send_sem=part_send.at[slot], recv_sem=part_recv.at[slot, where],
            device_id=away((-gap) % rows, 0), device_id_type=MESH,
        )

    plane_order = list(range(2, cols)) + [1]

    def step(offset, carry):
        j = count - 1 - offset
        slot, col_slot = j // rows, j // cols
        on_plane = my_row == lax.rem(j, rows)
        owner = on_plane & (my_col == lax.rem(j, cols))

        @pl.when(owner)
        def _():
            total[col_slot] = target_ref[col_slot] - total[col_slot]
            for where, gap in enumerate(gaps):
                @pl.when(j + gap < count)
                def _():
                    part_copy(col_slot, where, gap).wait_recv()
                    total[col_slot] = total[col_slot] - parts[col_slot, where]
            solved_ref[slot] = split_product(
                total[col_slot], weights[col_slot, 0], weights[col_slot, 1]
            )

            @pl.when(j + 1 < count)
            def _():
                chain_copy(slot, col_slot).wait_recv()
                solved_ref[slot] = solved_ref[slot] - split_product(
                    chain[col_slot], weights[col_slot, 2], weights[col_slot, 3]
                )

            @pl.when(j > 0)
            def _():
                chain_copy(slot, (j - 1) // cols).start()
            for o in plane_order:
                plane_copy(slot, o).start()

        @pl.when(on_plane & jnp.logical_not(owner))
        def _():
            plane_copy(slot, 1).wait_recv()

        @pl.when(on_plane)
        def _():
            for s in reversed(range(local_cols)):
                k = my_col + cols * s

                @pl.when(k < j - 1)
                def _():
                    total[s] = total[s] + split_product(
                        solved_ref[slot], *split(tiles_ref[slot, s])
                    )
                for where, gap in enumerate(gaps):
                    @pl.when(k == j - gap)
                    def _():
                        part_copy(s, where, gap).start()
        return carry

    lax.fori_loop(0, count, step, 0)

    def drain(offset, carry):
        j = count - 1 - offset
        slot = j // rows
        on_plane = my_row == lax.rem(j, rows)

        @pl.when(on_plane & (my_col == lax.rem(j, cols)))
        def _():
            @pl.when(j > 0)
            def _():
                chain_copy(slot, 0).wait_send()
            for o in plane_order:
                plane_copy(slot, o).wait_send()

        @pl.when(on_plane)
        def _():
            for s in range(local_cols):
                for where, gap in enumerate(gaps):
                    @pl.when(my_col + cols * s == j - gap)
                    def _():
                        part_copy(s, where, gap).wait_send()
        return carry

    lax.fori_loop(0, count, drain, 0)


def sweep(rows, cols, tiles, target, inverses, corrections):
    local_rows, local_cols, width = tiles.shape[0], tiles.shape[1], tiles.shape[2]
    rhs = target.shape[1]
    vmem = pl.BlockSpec(memory_space=pltpu.VMEM)
    dma = pltpu.SemaphoreType.DMA
    return pl.pallas_call(
        functools.partial(sweep_kernel, rows, cols),
        out_shape=jax.ShapeDtypeStruct((local_rows, rhs, width), jnp.float32),
        in_specs=[vmem] * (2 + 2 * local_cols),
        out_specs=vmem,
        scratch_shapes=[
            pltpu.VMEM((local_cols, rhs, width), jnp.float32),
            pltpu.VMEM((local_cols, rhs, width), jnp.float32),
            pltpu.VMEM((local_cols, rows - 1, rhs, width), jnp.float32),
            pltpu.VMEM((local_cols, 4, width, width), jnp.bfloat16),
            dma((local_rows,)),
            dma((local_rows, cols)),
            dma((local_cols,)),
            dma((local_cols,)),
            dma((local_rows,)),
            dma((local_cols, rows - 1)),
        ],
        compiler_params=pltpu.CompilerParams(collective_id=0, has_side_effects=True),
    )(tiles, target, *inverses, *corrections)


def body(factor_wide, factor_narrow, flags, forward_solution, solution_grad):
    row_count = lax.axis_size("row")
    col_count = lax.axis_size("col")
    my_row = lax.axis_index("row")
    my_col = lax.axis_index("col")
    local_rows = factor_wide.shape[0]
    local_cols = factor_wide.shape[2]
    tile_width = factor_wide.shape[4]
    tile_count = local_rows * row_count

    def pick(row_slot, col_slot):
        def cut(pool):
            return lax.dynamic_index_in_dim(pool[:, 0, col_slot, 0], row_slot, 0, keepdims=False)
        narrow = cut(flags) == 1
        return jnp.where(narrow, cut(factor_narrow).astype(jnp.float32), cut(factor_wide))

    targets = [my_col + col_count * s for s in range(local_cols)]
    holders = [
        (r, c) for r in range(row_count) for c in range(col_count)
        if any((c + col_count * s) % row_count == r for s in range(local_cols))
    ]
    to_holders = [
        ((r + 1) % row_count * col_count + c, r * col_count + c) for r, c in holders
    ]
    below = [None] * local_cols
    for s in reversed(range(local_cols)):
        tile = pick(jnp.minimum(targets[s] + 1, tile_count - 1) // row_count, s)
        below[s] = lax.ppermute(tile, ("row", "col"), to_holders)
    factor_tiles = jnp.where(
        flags[:, 0, :, 0, None, None] == 1,
        factor_narrow[:, 0, :, 0].astype(jnp.float32),
        factor_wide[:, 0, :, 0],
    )
    inverses = [invert(pick(j // row_count, s)) for s, j in enumerate(targets)]
    corrections = [
        jnp.dot(b, v, precision=PRODUCT_PRECISION, preferred_element_type=jnp.float32)
        for b, v in zip(below, inverses)
    ]
    target = jnp.swapaxes(solution_grad[:, 0], 1, 2)
    solved = sweep(row_count, col_count, factor_tiles, target, inverses, corrections)
    row_index = jnp.arange(local_rows, dtype=jnp.int32) * row_count + my_row
    col_index = jnp.arange(local_cols, dtype=jnp.int32) * col_count + my_col
    products = -jnp.einsum(
        "ark,blr->abkl", solved, forward_solution[:, 0], precision=PRODUCT_PRECISION
    )
    masks = lower_mask(row_index[:, None, None, None], col_index[None, :, None, None], tile_width)
    factor_grad = jnp.where(masks, products, jnp.zeros_like(products))
    return (jnp.swapaxes(solved, 1, 2)[:, None], factor_grad[:, None, :, None])


def solution(mesh):
    placed = (
        P(None, "row", None, "col", None, None),
        P(None, "row", None, "col", None, None),
        P(None, "row", None, "col"),
        P(None, "col", None, None),
        P(None, "col", None, None),
    )
    return jax.shard_map(
        body,
        mesh=mesh,
        in_specs=placed,
        out_specs=(P(None, "row", None, None), P(None, "row", None, "col", None, None)),
        check_vma=False,
    )
```
